256 devices in a mesh: asset: 16 (over y, x_hi, core), tm: 16 (over z, x_lo).
Axes of the slice: x: 4 (x_hi: 2, x_lo: 2; x = x_hi * 2 + x_lo), y: 4, z: 8, core: 2. Of those that a mesh axis runs over, the one named last changes fastest.
Arguments:
- day_ranks: int32 [224, 4096], P('tm', 'asset'), may hold values from 2 to 240
- confidence: float32 [224, 4096], P('tm', 'asset'), may hold values from 0.25 to 4
Outputs:
- correlation: bfloat16 [96, 4096, 4096], P('tm', 'asset')
The draws below stay inside these ranges and needn't reach their ends.
All inputs are finite; a program needn't handle non-finite values.
Results may differ from the reference program's by a relative error of at most 0.001.
Values sent between devices are 32-bit elements; how exact they have to be, the bound alone decides.
A program may use at most 64 MiB of HBM per device.

```python
import math
import jax
import jax.numpy as jnp
from jax import lax

ASSETS = 4096
WIN = 120
DAYS = 224
ENDS = 96
LEAD = 9


def touch_ends(values, key, low, high):
    index_at = [jax.random.randint(jax.random.fold_in(key, axis), (), 0, length) for axis, length in enumerate(values.shape)]
    longest = values.shape.index(max(values.shape))
    next_to = index_at[:longest] + [(index_at[longest] + 1) % values.shape[longest]] + index_at[longest + 1:]
    return values.at[tuple(index_at)].set(low).at[tuple(next_to)].set(high)


def shard_levels(key, extent, pieces, least, high):
    def one(dim, parts):
        steps = jax.random.uniform(jax.random.fold_in(jax.random.fold_in(key, 6), dim), (parts,), jnp.float32, least / len(pieces), high / len(pieces))
        return jnp.repeat(jnp.exp(steps), extent[dim] // parts).reshape((-1,) + (1,) * (len(extent) - dim - 1))

    level = one(*pieces[0])
    for cut in pieces[1:]:
        level = level * one(*cut)
    return level


def setup_inputs(seed: int = 0) -> dict:
    key_list = jax.random.split(jax.random.key(seed), 3)
    day_ranks = touch_ends(jax.random.randint(key_list[0], (DAYS, ASSETS), 2, 2 * WIN + 1), jax.random.fold_in(key_list[0], 1), 2, 2 * WIN).astype(jnp.int32)
    confidence = jnp.clip(jnp.exp(math.log(4.0) - 2.7725887 * jax.random.uniform(key_list[1], (DAYS, ASSETS), jnp.float32) ** shard_levels(key_list[1], (DAYS, ASSETS), ((0, 16), (1, 16)), -0.2, 0.2)), 0.25, 4.0)
    return {"day_ranks": day_ranks, "confidence": confidence}


epsilon = 1e-06

def reference(day_ranks, confidence):
    scores = confidence * (day_ranks - (WIN + 1)).astype(jnp.float32) / WIN

    def end_correlation(end_index):
        window_rows = lax.dynamic_slice_in_dim(scores, (end_index + LEAD).astype(jnp.int32), WIN, 0)
        window_mean = lax.optimization_barrier(jnp.sum(window_rows, 0)) / WIN
        centred = window_rows - window_mean[None, :]
        window_scale = lax.rsqrt(lax.optimization_barrier(jnp.sum(centred * centred, 0)) / WIN + epsilon)
        gram_sums = jnp.dot(window_rows.T, window_rows, precision=lax.Precision.HIGHEST, preferred_element_type=jnp.float32)
        centre = window_mean[:, None] * window_mean[None, :]
        spread = window_scale[:, None] * window_scale[None, :]
        return ((gram_sums / WIN - centre) * spread).astype(jnp.bfloat16)
    return lax.map(end_correlation, jnp.arange(ENDS, dtype=jnp.int32))
```

```python
import functools

import jax
import jax.numpy as jnp
from jax import lax
from jax.experimental import pallas as pl
from jax.experimental.pallas import tpu as pltpu
from jax.sharding import PartitionSpec as P

WIN = 120
ENDS_DEV = 6
SPAN = 125
LEAD = 9
HALF = 7
SLOTS = 10
PART = SLOTS * HALF
PIECES = 34
SEC = 144
DEPTH = 512
STOCKS = 256
BLOCKS = 16
epsilon = 1e-06
MESH = pl.DeviceIdType.MESH


def first_half(z):
    return jnp.minimum((LEAD + 12 * z) // HALF, 12)


def first_local(z, x_lo):
    g = first_half(z) - 2 * x_lo + 4
    return 2 * (g // 4 - 1) + jnp.minimum(g % 4, 2)


def gather_kernel(ranks_ref, conf_ref, g_ref, mine, zsend, zrecv, recv, send, csend, crecv):
    asset, tm = lax.axis_index("asset"), lax.axis_index("tm")
    core, x_hi, y = asset % 2, asset // 2 % 2, asset // 4
    z, x_lo = tm // 2, tm % 2
    x = x_hi * 2 + x_lo

    def chip(cx, cy):
        return ((cy * 2 + cx // 2) * 2 + core, z * 2 + cx % 2)

    def piece(cx, cy):
        return ((cy * 2 + cx // 2) * 2 + core) * 2 + cx % 2

    xs = [x, (x + 3) % 4, (x + 1) % 4, (x + 2) % 4]
    ys = [y, (y + 3) % 4, (y + 1) % 4, (y + 2) % 4]
    x_minus, x_plus = chip(xs[1], y), chip(xs[2], y)
    y_minus, y_plus = chip(x, ys[1]), chip(x, ys[2])
    partner = (asset + 1 - 2 * core, tm)
    line = [(asset, ((z + step) % 8) * 2 + x_lo) for step in range(1, 8)]

    barrier = pltpu.get_barrier_semaphore()
    for peer in line + [x_minus, x_plus, y_minus, y_plus, partner]:
        pl.semaphore_signal(barrier, inc=1, device_id=peer, device_id_type=MESH)

    scores = conf_ref[...] * (ranks_ref[...] - (WIN + 1)).astype(jnp.float32) / WIN
    for day in range(2 * HALF):
        for h in range(2):
            mine[day // HALF, day % HALF, h : h + 1, :] = scores[
                day : day + 1, h * 128 : (h + 1) * 128
            ]
    own = piece(x, y)
    first = first_local(z, x_lo)
    for b in range(2):
        slot = 2 * z + b - first

        @pl.when((slot >= 0) & (slot < SLOTS))
        def _():
            for day in range(HALF):
                for h in range(2):
                    g_ref[own, slot, day, h : h + 1, :] = scores[
                        b * HALF + day : b * HALF + day + 1, h * 128 : (h + 1) * 128
                    ]

    pl.semaphore_wait(barrier, 12)

    def z_copy(step, b):
        there = (z + step) % 8
        slot = 2 * z + b - first_local(there, x_lo)
        copy = pltpu.make_async_remote_copy(
            src_ref=mine.at[b],
            dst_ref=g_ref.at[own, jnp.clip(slot, 0, SLOTS - 1)],
            send_sem=zsend.at[2 * step + b],
            recv_sem=zrecv.at[jnp.clip(slot, 0, SLOTS - 1)],
            device_id=(asset, there * 2 + x_lo),
            device_id_type=MESH,
        )
        return (slot >= 0) & (slot < SLOTS), copy

    for step in (4, 3, 5, 2, 6, 1, 7):
        for b in range(2):
            go, copy = z_copy(step, b)
            pl.when(go)(copy.start)

    for slot in range(SLOTS):

        @pl.when((first + slot) // 2 != z)
        def _():
            pltpu.make_async_copy(mine.at[0], g_ref.at[own, slot], zrecv.at[slot]).wait()

    def part(cx, cy, low, high):
        return g_ref.at[piece(cx, cy), pl.ds(low, high - low)]

    def push(cx, cy, low, high, sem, peer):
        pltpu.make_async_remote_copy(
            src_ref=part(cx, cy, low, high),
            dst_ref=part(cx, cy, low, high),
            send_sem=send,
            recv_sem=recv.at[sem],
            device_id=peer,
            device_id_type=MESH,
        ).start()

    def arrived(cx, cy, low, high, sem):
        ref = part(cx, cy, low, high)
        pltpu.make_async_copy(ref, ref, recv.at[sem]).wait()

    def to_partner(cx, cy, low, high):
        pltpu.make_async_remote_copy(
            src_ref=part(cx, cy, low, high),
            dst_ref=part(cx, cy, low, high),
            send_sem=csend,
            recv_sem=crecv,
            device_id=partner,
            device_id_type=MESH,
        ).start()

    bounds = ((0, 3, 5), (5, 7, 10))

    def at(colour, i, j):
        return (xs[i], ys[j]) if colour == 0 else (xs[j], ys[i])

    peers = (((x_minus, x_plus), (y_minus, y_plus)), ((y_minus, y_plus), (x_minus, x_plus)))

    def sem_of(colour, stage, i, k):
        return colour * 20 + (k if stage == 0 else 4 + 4 * i + k)

    def start_ring(colour, stage, i):
        low, _, high = bounds[colour]
        minus, plus = peers[colour][stage]
        cx, cy = at(colour, i, 0)
        push(cx, cy, low, high, sem_of(colour, stage, place_there(i, stage), 0), plus)
        push(cx, cy, low, high, sem_of(colour, stage, place_there(i, stage), 1), minus)

    def place_there(i, stage):
        return i

    def step_ring(colour, stage, i, side):
        low, mid, high = bounds[colour]
        minus, plus = peers[colour][stage]
        cx, cy = at(colour, side, 0) if stage == 0 else at(colour, i, side)
        arrived(cx, cy, low, high, sem_of(colour, stage, i, side - 1))
        if side == 1:
            push(cx, cy, low, mid, sem_of(colour, stage, i, 2), plus)
        else:
            push(cx, cy, mid, high, sem_of(colour, stage, i, 3), minus)
        to_partner(cx, cy, low, high)

    def end_ring(colour, stage, i):
        low, mid, high = bounds[colour]
        cx, cy = at(colour, 3, 0) if stage == 0 else at(colour, i, 3)
        arrived(cx, cy, low, mid, sem_of(colour, stage, i, 2))
        arrived(cx, cy, mid, high, sem_of(colour, stage, i, 3))
        to_partner(cx, cy, low, high)

    for colour in range(2):
        start_ring(colour, 0, 0)
    for colour in range(2):
        start_ring(colour, 1, 0)
    for colour in range(2):
        low, _, high = bounds[colour]
        to_partner(x, y, low, high)
    for side in (1, 2):
        for colour in range(2):
            step_ring(colour, 0, 0, side)
            start_ring(colour, 1, side)
    for side in (1, 2):
        for colour in range(2):
            step_ring(colour, 1, 0, side)
    for colour in range(2):
        end_ring(colour, 0, 0)
        start_ring(colour, 1, 3)
    for i in (1, 2):
        for side in (1, 2):
            for colour in range(2):
                step_ring(colour, 1, i, side)
    for colour in range(2):
        end_ring(colour, 1, 0)
    for side in (1, 2):
        for colour in range(2):
            step_ring(colour, 1, 3, side)
    for i in (1, 2, 3):
        for colour in range(2):
            end_ring(colour, 1, i)

    for step in range(1, 8):
        for b in range(2):
            go, copy = z_copy(step, b)
            pl.when(go)(copy.wait_send)
    whole = g_ref.at[pl.ds(0, 15)]
    pltpu.make_async_copy(whole, whole, send).wait()
    whole = g_ref.at[pl.ds(0, 16)]
    pltpu.make_async_copy(whole, whole, csend).wait()
    pltpu.make_async_copy(whole, whole, crecv).wait()


def gather(day_ranks, confidence):
    shape = (PIECES, SLOTS, HALF, 2, 128)
    return pl.pallas_call(
        gather_kernel,
        out_shape=jax.ShapeDtypeStruct(shape, jnp.float32),
        in_specs=[pl.BlockSpec(memory_space=pltpu.VMEM)] * 2,
        out_specs=pl.BlockSpec(memory_space=pltpu.VMEM),
        scratch_shapes=[
            pltpu.VMEM((2, HALF, 2, 128), jnp.float32),
            pltpu.SemaphoreType.DMA((16,)),
            pltpu.SemaphoreType.DMA((SLOTS,)),
            pltpu.SemaphoreType.DMA((40,)),
            pltpu.SemaphoreType.DMA,
            pltpu.SemaphoreType.DMA,
            pltpu.SemaphoreType.DMA,
        ],
        compiler_params=pltpu.CompilerParams(
            collective_id=0, has_side_effects=True, vmem_limit_bytes=16 * 2**20
        ),
        name="gather",
    )(day_ranks, confidence)


def correlate_kernel(g_ref, out_ref, left, right, offset, mean_scale):
    step = pl.program_id(0)
    tm = lax.axis_index("tm")
    z = tm // 2
    rows = g_ref

    def load(block):
        lists = []
        for x_lo in range(2):
            base = (block * 2 + x_lo) * PART * 2
            halves = [rows[pl.ds(base + h, SEC // 2, 2), :] for h in range(2)]
            lists.append(jnp.concatenate(halves, 1))
        return jnp.concatenate(lists, 0)

    @pl.when(step == 0)
    def _():
        row = lax.broadcasted_iota(jnp.int32, (SEC, STOCKS), 0)
        x_lo = (row >= SEC // 2).astype(jnp.int32)
        inner = row - x_lo * (SEC // 2)
        local = (inner * 37) >> 8
        q = jnp.where(x_lo == 0, first_local(z, 0), first_local(z, 1)) + local
        day = HALF * (4 * (q >> 1) + 2 * x_lo + (q & 1)) + inner - HALF * local
        off = day - (LEAD + ENDS_DEV * tm)
        offset[...] = jnp.where(inner < PART, off, -1).astype(jnp.float32)
        right[3 * SEC :, :] = jnp.zeros((DEPTH - 3 * SEC, STOCKS), jnp.bfloat16)

    off = offset[...]

    def centred(block):
        values = load(block)
        common = (off >= ENDS_DEV - 1) & (off < WIN)
        centre = jnp.sum(jnp.where(common, values, 0.0), 0, keepdims=True) / (WIN - ENDS_DEV + 1)
        return jnp.where((off >= 0) & (off < SPAN), values - centre, 0.0)

    def moments(values):
        square = values * values
        out = []
        for e in range(ENDS_DEV):
            inside = (off >= e) & (off < e + WIN)
            mean = jnp.sum(jnp.where(inside, values, 0.0), 0, keepdims=True) / WIN
            power = jnp.sum(jnp.where(inside, square, 0.0), 0, keepdims=True) / WIN
            out.append((mean, lax.rsqrt(power - mean * mean + epsilon)))
        return out

    def split(values):
        high = values.astype(jnp.bfloat16)
        return high, (values - high.astype(jnp.float32)).astype(jnp.bfloat16)

    @pl.when(step == 0)
    def _():
        values = centred(lax.axis_index("asset"))
        for e, (mean, scale) in enumerate(moments(values)):
            inside = (off >= e) & (off < e + WIN)
            unit = jnp.where(inside, (values - mean) * (scale / WIN), 0.0)
            high, low = split(unit)
            zero = jnp.zeros((DEPTH - 3 * SEC, STOCKS), jnp.bfloat16)
            stacked = jnp.concatenate([high, high, low, zero], 0)
            left[e * STOCKS : (e + 1) * STOCKS, :] = stacked.T

    values = centred(step)
    high, low = split(values)
    right[0:SEC, :] = high
    right[SEC : 2 * SEC, :] = low
    right[2 * SEC : 3 * SEC, :] = high
    for e, (_, scale) in enumerate(moments(values)):
        gram = jnp.dot(
            left[e * STOCKS : (e + 1) * STOCKS, :],
            right[...],
            preferred_element_type=jnp.float32,
        )
        out_ref[e] = (gram * scale).astype(jnp.bfloat16)


def correlate(rows):
    return pl.pallas_call(
        correlate_kernel,
        grid=(BLOCKS,),
        out_shape=jax.ShapeDtypeStruct((ENDS_DEV, STOCKS, STOCKS * BLOCKS), jnp.bfloat16),
        in_specs=[pl.BlockSpec(memory_space=pltpu.VMEM)],
        out_specs=pl.BlockSpec((ENDS_DEV, STOCKS, STOCKS), lambda a: (0, 0, a)),
        scratch_shapes=[
            pltpu.VMEM((ENDS_DEV * STOCKS, DEPTH), jnp.bfloat16),
            pltpu.VMEM((DEPTH, STOCKS), jnp.bfloat16),
            pltpu.VMEM((SEC, STOCKS), jnp.float32),
            pltpu.VMEM((16, STOCKS), jnp.float32),
        ],
        compiler_params=pltpu.CompilerParams(vmem_limit_bytes=32 * 2**20),
        cost_estimate=pl.CostEstimate(
            flops=2 * 1536 * 4096 * 512, bytes_accessed=15 * 10**6, transcendentals=0
        ),
        name="correlate",
    )(rows)


def per_device(day_ranks, confidence):
    pieces = gather(day_ranks, confidence)
    return correlate(pieces.reshape(PIECES * PART * 2, 128))


def solution(mesh):
    return jax.shard_map(
        per_device,
        mesh=mesh,
        in_specs=(P("tm", "asset"), P("tm", "asset")),
        out_specs=P("tm", "asset", None),
        check_vma=False,
    )
```
